32 devices in a mesh: op: 4 (over z), row: 8 (over y, x, core).
Axes of the slice: x: 2, y: 2, z: 4, core: 2. Of those that a mesh axis runs over, the one named last changes fastest.
Arguments:
- wannier_ops: bfloat16 [2, 1000, 2, 128, 128], P(None, 'row'), may hold values from -0.1875 to 0.1875
- r_coords: int32 [1000, 3], P('row'), may hold values from -8 to 8
- degeneracy: int32 [1000], P('row'), may hold values from 1 to 4
- kpoints: int32 [64, 3], replicated, may hold values from 0 to 15
- bloch_vectors: bfloat16 [64, 2, 64, 128], P(('op', 'row')), may hold values from -0.375 to 0.375
Outputs:
- covariant: float32 [64, 2, 4096], P(('op', 'row'))
The draws below stay inside these ranges and needn't reach their ends.
Inputs may be any that keep to these rules, and one draw needn't show every extreme that they name: `r_coords`: these coordinates are small integers; a program may pack several of them into one int32 word when it moves them. `degeneracy`: these degeneracies are small integers; a program may pack several of them into one int32 word when it moves them.
All inputs are finite; a program needn't handle non-finite values.
Results may differ from the reference program's by a relative error of at most 0.0038.
Values may be sent and summed in bfloat16 or wider, within the bound.
A program may use at most 192 MiB of HBM per device.

```python
import math
import jax
import jax.numpy as jnp
from jax import lax

W = 128
NB = 64
GRID = 16
RMAX = 8
NR = 1000
K = 64


def place_ends(entries, rng, least, top_value):
    longest = entries.shape.index(max(entries.shape))
    spots = []
    for shift in (0, 1):
        where = [jax.random.randint(jax.random.fold_in(rng, axis), (), 0, length) for axis, length in enumerate(entries.shape)]
        where[longest] = (where[longest] + shift) % entries.shape[longest]
        spots.append(tuple(where))
    return entries.at[spots[0]].set(least).at[spots[1]].set(top_value)


def block_levels(key, dims, split, smallest, high):
    factor_of, own = 1.0, jax.random.fold_in(key, 6)
    for position, parts in split:
        heights = jnp.exp(jax.random.uniform(jax.random.fold_in(own, position), (parts,), jnp.float32, smallest / len(split), high / len(split)))
        factor_of = factor_of * jnp.repeat(heights, dims[position] // parts).reshape([-1 if axis == position else 1 for axis in range(len(dims))])
    return factor_of


def scatter_about(rng, shape, scale, most, split=(), kind=jnp.bfloat16):
    drawn = jax.random.normal(rng, shape, jnp.float32) * scale
    if len(split) > 0:
        drawn = block_levels(rng, shape, split, -0.22, 0.18) * drawn
    return jnp.clip(drawn, min=-most, max=most).astype(kind)


def setup_inputs(seed: int = 0) -> dict:
    key_of = jax.random.split(jax.random.key(seed), 6)
    wannier_ops = scatter_about(key_of[0], (2, NR, 2, W, W), NR ** -0.5, 0.1875, ((1, 8),))
    r_coords = place_ends(jax.random.randint(key_of[1], (NR, 3), -RMAX, RMAX + 1), jax.random.fold_in(key_of[1], 1), -RMAX, RMAX).astype(jnp.int32)
    degeneracy = place_ends(jax.random.randint(key_of[2], (NR,), 1, 5), jax.random.fold_in(key_of[2], 1), 1, 4).astype(jnp.int32)
    kpoints = place_ends(jax.random.randint(key_of[3], (K, 3), 0, GRID), jax.random.fold_in(key_of[3], 1), 0, GRID - 1).astype(jnp.int32)
    bloch_vectors = scatter_about(key_of[4], (K, 2, NB, W), (2 * W) ** -0.5, 0.375, ((0, 32),))
    return dict(wannier_ops=wannier_ops, r_coords=r_coords, degeneracy=degeneracy, kpoints=kpoints, bloch_vectors=bloch_vectors)


TWO_PI = 6.283185307179586
HIGH = lax.Precision.HIGHEST

def phase_parts(r_coords, degeneracy, kpoints):
    turns_int = lax.optimization_barrier(jnp.sum(r_coords[:, None, :] * kpoints[None, :, :], axis=2)) % GRID
    angles = turns_int.astype(jnp.float32) * (TWO_PI / GRID)
    weights = 1.0 / degeneracy.astype(jnp.float32)
    cosine = jnp.cos(angles) * weights[:, None]
    sine_part = jnp.sin(angles) * weights[:, None]
    along_x = (r_coords[:, 0].astype(jnp.float32) / RMAX)[:, None]
    return (cosine, sine_part, along_x)

def fourier(phase_re, phase_im, flat_ops):
    stacked = jnp.concatenate([phase_re, phase_im], axis=1)
    product_sum = lax.dot_general(stacked, flat_ops, (((0,), (0,)), ((), ())), preferred_element_type=jnp.float32)
    k_count = phase_re.shape[1]
    half_cols = flat_ops.shape[1] // 2
    real_part = product_sum[:k_count, :half_cols] - product_sum[k_count:, half_cols:]
    imag_part = product_sum[:k_count, half_cols:] + product_sum[k_count:, :half_cols]
    return (real_part, imag_part)

def complex_mul(form, left, right):

    def single(first, second):
        return jnp.einsum(form, first, second, precision=HIGH)
    return (single(left[0], right[0]) - single(left[1], right[1]), single(left[0], right[1]) + single(left[1], right[0]))

def rotate(op_pair, vec_pair):
    left_side = complex_mul('knm,kmp->knp', (vec_pair[0], -vec_pair[1]), op_pair)
    return complex_mul('knm,kpm->knp', left_side, vec_pair)

def covariant_form(ham, deriv, posit, posit_deriv):
    band_count = ham[0].shape[-1]
    factor = 1.0 / math.sqrt(band_count)
    form = 'kab,kbc->kac'
    a_d = complex_mul(form, posit, deriv)
    d_a = complex_mul(form, deriv, posit)
    h_a = complex_mul(form, ham, posit)
    a_h = complex_mul(form, posit, ham)
    g_real = posit_deriv[0] + factor * (h_a[0] + a_h[0] - (a_d[1] - d_a[1]))
    g_imag = posit_deriv[1] + factor * (h_a[1] + a_h[1] + (a_d[0] - d_a[0]))
    k_count = g_real.shape[0]
    return jnp.stack([g_real.reshape(k_count, -1), g_imag.reshape(k_count, -1)], axis=1)

def reference(wannier_ops, r_coords, degeneracy, kpoints, bloch_vectors):
    cosine, sine_part, along_x = phase_parts(r_coords, degeneracy, kpoints)
    vectors = bloch_vectors.astype(jnp.float32)
    vec_pair = (vectors[:, 0], vectors[:, 1])
    rotated = []
    for component_id in range(4):
        flat_ops = wannier_ops[component_id // 2].reshape(NR, 2 * W * W)
        if component_id % 2 == 1:
            phase_re = -along_x * sine_part
            phase_im = along_x * cosine
        else:
            phase_re = cosine
            phase_im = sine_part
        real_part, imag_part = fourier(phase_re.astype(jnp.bfloat16), phase_im.astype(jnp.bfloat16), flat_ops)
        rotated.append(rotate((real_part.reshape(K, W, W), imag_part.reshape(K, W, W)), vec_pair))
    return covariant_form(rotated[0], rotated[1], rotated[2], rotated[3])
```

```python
import functools
import math

import jax
import jax.numpy as jnp
from jax import lax
from jax.experimental import pallas as pl
from jax.experimental.pallas import tpu as pltpu
from jax.sharding import PartitionSpec as P

GRID = 16
RMAX = 8
TWO_PI = 6.283185307179586
PIECE = 4
SPAN = 4
UNROLL = 2
FOLD = 4 * PIECE
MESH = pl.DeviceIdType.MESH
F32 = jnp.float32
BF16 = jnp.bfloat16
NT = (((1,), (1,)), ((), ()))
NN = (((1,), (0,)), ((), ()))
TN = (((0,), (0,)), ((), ()))


def mm(a, b, dims=NN):
    return lax.dot_general(a, b, dims, preferred_element_type=F32)


def split(x):
    high = x.astype(BF16)
    return high, (x - high.astype(F32)).astype(BF16)


def iota(shape, axis):
    return lax.broadcasted_iota(jnp.int32, shape, axis)


def kernel(
    n, ops_ref, rc_ref, deg_ref, kp_ref, v_ref, out_ref,
    obuf, rci, degi, kpi, rcs, kps, inners, picked, spread, left4,
    fown, fsend, frecv, vall, sbuf, rbuf, own,
    osem, isem, fs, fr, vs, vr, bs, br,
):
    me = lax.axis_index("row")
    group = lax.axis_index("op")
    core = lax.rem(me, 2)
    chip = me // 2
    partner = me + 1 - 2 * core
    chips = n // 2
    r_local, width = ops_ref.shape[1], ops_ref.shape[-1]
    r_pad = rcs.shape[1]
    pieces = width // PIECE
    steps = pieces // SPAN
    depth = 2 * PIECE * r_pad
    per, _, bands, _ = v_ref.shape
    slots = chips * per
    k_group = n * per
    half = slots * FOLD
    flat = obuf.reshape(2 * pieces * depth, width)

    def peer(s):
        return lax.rem(me + 2 * s, n)

    barrier = pltpu.get_barrier_semaphore()
    pl.semaphore_signal(barrier, inc=1, device_id={"row": partner}, device_id_type=MESH)
    for s in range(1, chips):
        pl.semaphore_signal(barrier, inc=1, device_id={"row": peer(s)}, device_id_type=MESH)

    small = [
        pltpu.make_async_copy(src, dst, isem.at[i])
        for i, (src, dst) in enumerate(
            ((kp_ref, kpi), (rc_ref, rci), (deg_ref, degi), (v_ref, vall.at[chip]))
        )
    ]
    for copy in small:
        copy.start()

    def op_copy(q):
        return pltpu.make_async_copy(
            ops_ref.at[q // pieces, :, :, q % pieces],
            obuf.at[q // pieces, q % pieces, pl.ds(0, r_local)],
            osem.at[q],
        )

    def op_start(q, carry):
        op_copy(q).start()
        return carry

    lax.fori_loop(0, 2 * pieces, op_start, 0, unroll=4)

    if r_pad > r_local:
        tail = 2 * PIECE * (r_pad - r_local)

        def clear(q, carry):
            flat[pl.ds(pl.multiple_of(q * depth, depth) + 2 * PIECE * r_local, tail), :] = jnp.zeros(
                (tail, width), BF16
            )
            return carry

        lax.fori_loop(0, 2 * pieces, clear, 0, unroll=4)

    for p in range(2):
        spread[pl.ds(p * r_pad, r_pad), :] = jnp.where(
            iota((r_pad, depth), 1) // PIECE == 2 * iota((r_pad, depth), 0) + p, 1.0, 0.0
        ).astype(BF16)
    rcs[...] = jnp.zeros_like(rcs)
    kps[...] = jnp.zeros_like(kps)

    for copy in small[:3]:
        copy.wait()
    rcs[pl.ds(0, 3), pl.ds(0, r_local)] = rci[...].astype(F32)
    kps[pl.ds(0, 3), :] = kpi[...].astype(F32)
    weights = jnp.concatenate(
        [1.0 / degi[...].astype(F32), jnp.zeros((1, r_pad - r_local), F32)], axis=1
    ) if r_pad > r_local else 1.0 / degi[...].astype(F32)
    inners[...] = mm(kps[...].astype(BF16), rcs[...].astype(BF16), TN)
    for h in range(2):
        for c in range(chips):
            owner = 2 * c + lax.rem(core + h, 2)
            picked[pl.ds((h * chips + c) * per, per), :] = inners[
                pl.ds(group * k_group + owner * per, per), :
            ]
    inner = picked[...]
    along_x = rcs[pl.ds(0, 1), :] / RMAX
    turns = inner - GRID * jnp.floor(inner / GRID)
    angles = turns * (TWO_PI / GRID)
    cosine = jnp.cos(angles) * weights
    sine = jnp.sin(angles) * weights
    parts = []
    for re, im in ((cosine, sine), (-along_x * sine, along_x * cosine)):
        parts.append(jnp.concatenate([re, -im], axis=1).astype(BF16))
        parts.append(jnp.concatenate([im, re], axis=1).astype(BF16))
    phases = jnp.concatenate(parts, axis=0)

    for h in range(2):
        row = iota((half, 4 * k_group), 0) + h * half
        source = (
            ((row // PIECE) % 2) * (2 * k_group) + ((row // (2 * PIECE)) % 2) * k_group + row // FOLD
        )
        chosen = jnp.where(iota((half, 4 * k_group), 1) == source, 1.0, 0.0).astype(BF16)
        ordered = mm(chosen, phases).astype(BF16)
        wide = mm(ordered, spread[...])
        same = iota((half, depth), 0) % PIECE == iota((half, depth), 1) % PIECE
        left4[pl.ds(h * half, half), :] = jnp.where(same, wide, 0.0).astype(BF16)

    small[3].wait()
    pl.semaphore_wait(barrier, chips)

    def v_copy(s):
        to = peer(s)
        return pltpu.make_async_remote_copy(
            src_ref=vall.at[chip], dst_ref=vall.at[chip],
            send_sem=vs.at[to // 2], recv_sem=vr.at[chip],
            device_id={"row": to}, device_id_type=MESH,
        )

    for s in range(1, chips):
        v_copy(s).start()

    def v_wait(s):
        src = peer(s)
        pltpu.make_async_remote_copy(
            src_ref=vall.at[chip], dst_ref=vall.at[src // 2],
            send_sem=vs.at[src // 2], recv_sem=vr.at[src // 2],
            device_id={"row": src}, device_id_type=MESH,
        ).wait()

    def f_copy(t):
        return pltpu.make_async_remote_copy(
            src_ref=fsend.at[t], dst_ref=frecv.at[t], send_sem=fs.at[t], recv_sem=fr.at[t],
            device_id={"row": partner}, device_id_type=MESH,
        )

    def fourier(op):
        def body(i, carry):
            for u in range(UNROLL):
                t = op * steps + i * UNROLL + u
                for q in range(SPAN):
                    op_copy(t * SPAN + q).wait()
            for u in range(UNROLL):
                t = op * steps + i * UNROLL + u
                tiles = [
                    flat[pl.ds(pl.multiple_of((t * SPAN + q) * depth, depth), depth), :]
                    for q in range(SPAN)
                ]
                got = mm(left4[...], jnp.concatenate(tiles, axis=1))
                fown[t] = got[:half]
                fsend[t] = got[half:].astype(BF16)
            for u in range(UNROLL):
                f_copy(op * steps + i * UNROLL + u).start()
            return carry

        lax.fori_loop(0, steps // UNROLL, body, 0)

    def f_wait(op):
        def body(i, carry):
            f_copy(op * steps + i).wait()
            return carry

        lax.fori_loop(0, steps, body, 0)

    upper = iota((2 * PIECE, width), 0) < PIECE

    def band_blocks(op, owner, kk):
        slot = owner * per + kk
        v_re, v_im = vall[owner, kk, 0], vall[owner, kk, 1]
        first = jnp.concatenate([v_re, -v_im], axis=1)
        second = jnp.concatenate([v_im, v_re], axis=1)
        third = jnp.concatenate([-v_re, v_im], axis=1)
        right = jnp.concatenate([first, second, second, third], axis=0)
        rows = pl.ds(pl.multiple_of(slot * FOLD, FOLD), FOLD)
        cells = [[[], []], [[], []]]
        for t in range(op * steps, (op + 1) * steps):
            total = fown[t, rows, :] + frecv[t, rows, :].astype(F32)
            for q in range(0, SPAN, 2):
                for part in range(2):
                    low = total[part * 8:part * 8 + 8, q * width:(q + 1) * width]
                    high = total[part * 8:part * 8 + 8, (q + 1) * width:(q + 2) * width]
                    cells[0][part].append(jnp.where(upper, low, pltpu.roll(high, PIECE, 0)))
                    cells[1][part].append(jnp.where(upper, pltpu.roll(low, PIECE, 0), high))
        lefts = [
            jnp.concatenate([jnp.concatenate(cells[c][part], axis=0) for part in range(2)], axis=1)
            for c in range(2)
        ]
        high, low = split(jnp.concatenate(lefts, axis=0))
        g = (mm(high, right, NT) + mm(low, right, NT)).astype(BF16)
        cols = 2 * bands
        stacks = [
            jnp.concatenate(
                [g[c * width:(c + 1) * width, :cols], g[c * width:(c + 1) * width, cols:]], axis=0
            )
            for c in range(2)
        ]
        b = mm(jnp.concatenate([v_re, v_im], axis=1), jnp.concatenate(stacks, axis=1))
        return b[:, :cols], b[:, cols:]

    def b_copy(op, kk, s):
        to = peer(s)
        return pltpu.make_async_remote_copy(
            src_ref=sbuf.at[op, kk, to // 2], dst_ref=rbuf.at[op, kk, chip],
            send_sem=bs.at[op, kk, to // 2], recv_sem=br.at[op, kk, chip],
            device_id={"row": to}, device_id_type=MESH,
        )

    def b_wait(op, kk, s):
        src = peer(s)
        pltpu.make_async_remote_copy(
            src_ref=sbuf.at[op, kk, src // 2], dst_ref=rbuf.at[op, kk, src // 2],
            send_sem=bs.at[op, kk, src // 2], recv_sem=br.at[op, kk, src // 2],
            device_id={"row": src}, device_id_type=MESH,
        ).wait()

    def bands_out(op):
        def body(kk, carry):
            for s in range(1, chips):
                to = peer(s) // 2
                for comp, b in enumerate(band_blocks(op, to, kk)):
                    sbuf[op, kk, to, comp] = b.astype(BF16)
            for s in range(1, chips):
                b_copy(op, kk, s).start()
            return carry

        lax.fori_loop(0, per, body, 0)

    def bands_own(op):
        for kk in range(per):
            for comp, b in enumerate(band_blocks(op, chip, kk)):
                own[op, kk, comp] = b

    fourier(0)
    for s in range(1, chips):
        v_wait(s)
    f_wait(0)
    bands_out(0)
    fourier(1)
    bands_own(0)
    f_wait(1)
    bands_out(1)
    bands_own(1)

    factor = 1.0 / math.sqrt(bands)

    def turn(m):
        return jnp.concatenate([-m[:, bands:], m[:, :bands]], axis=1)

    for kk in range(per):
        for op in range(2):
            for s in range(1, chips):
                b_wait(op, kk, s)
        sums = []
        for op in range(2):
            for comp in range(2):
                total = own[op, kk, comp]
                for s in range(1, chips):
                    total = total + rbuf[op, kk, peer(s) // 2, comp].astype(F32)
                sums.append(total)
        ham, deriv, posit, last = sums
        i_deriv = turn(deriv)
        plus, minus = ham + i_deriv, ham - i_deriv
        lh, ll = split(jnp.concatenate([posit, minus], axis=1))
        rh, rl = split(jnp.concatenate([plus, turn(plus), posit, turn(posit)], axis=0))
        prod = mm(
            jnp.concatenate([lh, lh, ll], axis=1), jnp.concatenate([rh, rl, rh], axis=0)
        )
        res = last + factor * prod
        out_ref[kk, 0] = res[:, :bands]
        out_ref[kk, 1] = res[:, bands:]


def on_device(wannier_ops, r_coords, degeneracy, kpoints, bloch_vectors):
    n = lax.axis_size("row")
    chips = n // 2
    r_local, width = wannier_ops.shape[1], wannier_ops.shape[-1]
    per, _, bands, _ = bloch_vectors.shape
    r_pad = -(-r_local // 128) * 128
    pieces = width // PIECE
    steps = 2 * (pieces // SPAN)
    depth = 2 * PIECE * r_pad
    half = chips * per * FOLD
    ks = kpoints.shape[0]
    vmem = pl.BlockSpec(memory_space=pltpu.VMEM)
    far = pl.BlockSpec(memory_space=pl.ANY)
    dma = pltpu.SemaphoreType.DMA
    res = pl.pallas_call(
        functools.partial(kernel, n),
        out_shape=jax.ShapeDtypeStruct((per, 2, bands, bands), F32),
        in_specs=[far] * 5,
        out_specs=vmem,
        scratch_shapes=[
            pltpu.VMEM((2, pieces, r_pad, 2, PIECE, width), BF16),
            pltpu.VMEM((3, r_local), jnp.int32),
            pltpu.VMEM((1, r_local), jnp.int32),
            pltpu.VMEM((3, ks), jnp.int32),
            pltpu.VMEM((8, r_pad), F32),
            pltpu.VMEM((8, ks), F32),
            pltpu.VMEM((ks, r_pad), F32),
            pltpu.VMEM((n * per, r_pad), F32),
            pltpu.VMEM((2 * r_pad, depth), BF16),
            pltpu.VMEM((2 * half, depth), BF16),
            pltpu.VMEM((steps, half, SPAN * width), F32),
            pltpu.VMEM((steps, half, SPAN * width), BF16),
            pltpu.VMEM((steps, half, SPAN * width), BF16),
            pltpu.VMEM((chips, per, 2, bands, width), BF16),
            pltpu.VMEM((2, per, chips, 2, bands, 2 * bands), BF16),
            pltpu.VMEM((2, per, chips, 2, bands, 2 * bands), BF16),
            pltpu.VMEM((2, per, 2, bands, 2 * bands), F32),
            dma((2 * pieces,)),
            dma((4,)),
            dma((steps,)),
            dma((steps,)),
            dma((chips,)),
            dma((chips,)),
            dma((2, per, chips)),
            dma((2, per, chips)),
        ],
        compiler_params=pltpu.CompilerParams(
            collective_id=0, has_side_effects=True, vmem_limit_bytes=62 * 1024 * 1024
        ),
    )(
        wannier_ops.reshape(2, r_local, 2, pieces, PIECE, width),
        r_coords.T, degeneracy.reshape(1, r_local), kpoints.T, bloch_vectors,
    )
    return res.reshape(per, 2, bands * bands)


def solution(mesh):
    in_specs = (
        P(None, "row", None, None, None),
        P("row", None),
        P("row"),
        P(),
        P(("op", "row"), None, None, None),
    )
    out_specs = P(("op", "row"), None, None)
    return jax.shard_map(
        on_device, mesh=mesh, in_specs=in_specs, out_specs=out_specs, check_vma=False
    )
```

```python
import functools
import math

import jax
import jax.numpy as jnp
from jax import lax
from jax.experimental import pallas as pl
from jax.experimental.pallas import tpu as pltpu
from jax.sharding import PartitionSpec as P

GRID = 16
RMAX = 8
TWO_PI = 6.283185307179586
PIECE = 4
SPAN = 4
UNROLL = 2
LOT = 3
EARLY = 24
FOLD = 4 * PIECE
MESH = pl.DeviceIdType.MESH
F32 = jnp.float32
BF16 = jnp.bfloat16
NT = (((1,), (1,)), ((), ()))
NN = (((1,), (0,)), ((), ()))
TN = (((0,), (0,)), ((), ()))


def mm(a, b, dims=NN):
    return lax.dot_general(a, b, dims, preferred_element_type=F32)


def split(x):
    high = x.astype(BF16)
    return high, (x - high.astype(F32)).astype(BF16)


def iota(shape, axis):
    return lax.broadcasted_iota(jnp.int32, shape, axis)


def kernel(
    n, ops_ref, rc_ref, deg_ref, kp_ref, v_ref, out_ref,
    obuf, rci, degi, kpi, rcs, kps, inners, picked, spread, left4,
    fown, fsend, frecv, vall, sbuf, rbuf, own,
    osem, isem, fs, fr, vs, vr, bs, br,
):
    me = lax.axis_index("row")
    group = lax.axis_index("op")
    core = lax.rem(me, 2)
    chip = me // 2
    partner = me + 1 - 2 * core
    chips = n // 2
    r_local, width = ops_ref.shape[1], ops_ref.shape[-1]
    r_pad = rcs.shape[1]
    pieces = width // PIECE
    steps = pieces // SPAN
    depth = 2 * PIECE * r_pad
    per, _, bands, _ = v_ref.shape
    slots = chips * per
    k_group = n * per
    half = slots * FOLD
    flat = obuf.reshape(2 * pieces * depth, width)

    def peer(s):
        return lax.rem(me + 2 * s, n)

    barrier = pltpu.get_barrier_semaphore()
    pl.semaphore_signal(barrier, inc=1, device_id={"row": partner}, device_id_type=MESH)
    for s in range(1, chips):
        pl.semaphore_signal(barrier, inc=1, device_id={"row": peer(s)}, device_id_type=MESH)

    small = [
        pltpu.make_async_copy(src, dst, isem.at[i])
        for i, (src, dst) in enumerate(
            ((kp_ref, kpi), (rc_ref, rci), (deg_ref, degi), (v_ref, vall.at[chip]))
        )
    ]
    for copy in small:
        copy.start()

    def op_copy(q):
        return pltpu.make_async_copy(
            ops_ref.at[q // pieces, :, :, q % pieces],
            obuf.at[q // pieces, q % pieces, pl.ds(0, r_local)],
            osem.at[q],
        )

    early = min(EARLY, 2 * pieces)
    for q in range(early):
        op_copy(q).start(priority=1)

    if r_pad > r_local:
        tail = 2 * PIECE * (r_pad - r_local)

        def clear(q, carry):
            flat[pl.ds(pl.multiple_of(q * depth, depth) + 2 * PIECE * r_local, tail), :] = jnp.zeros(
                (tail, width), BF16
            )
            return carry

        lax.fori_loop(0, 2 * pieces, clear, 0, unroll=4)

    for p in range(2):
        spread[pl.ds(p * r_pad, r_pad), :] = jnp.where(
            iota((r_pad, depth), 1) // PIECE == 2 * iota((r_pad, depth), 0) + p, 1.0, 0.0
        ).astype(BF16)
    rcs[...] = jnp.zeros_like(rcs)
    kps[...] = jnp.zeros_like(kps)

    for copy in small[:3]:
        copy.wait()
    rcs[pl.ds(0, 3), pl.ds(0, r_local)] = rci[...].astype(F32)
    kps[pl.ds(0, 3), :] = kpi[...].astype(F32)
    weights = jnp.concatenate(
        [1.0 / degi[...].astype(F32), jnp.zeros((1, r_pad - r_local), F32)], axis=1
    ) if r_pad > r_local else 1.0 / degi[...].astype(F32)
    inners[...] = mm(kps[...].astype(BF16), rcs[...].astype(BF16), TN)
    for h in range(2):
        for c in range(chips):
            owner = 2 * c + lax.rem(core + h, 2)
            picked[pl.ds((h * chips + c) * per, per), :] = inners[
                pl.ds(group * k_group + owner * per, per), :
            ]
    inner = picked[...]
    along_x = rcs[pl.ds(0, 1), :] / RMAX
    turns = inner - GRID * jnp.floor(inner / GRID)
    angles = turns * (TWO_PI / GRID)
    cosine = jnp.cos(angles) * weights
    sine = jnp.sin(angles) * weights
    parts = []
    for re, im in ((cosine, sine), (-along_x * sine, along_x * cosine)):
        parts.append(jnp.concatenate([re, -im], axis=1).astype(BF16))
        parts.append(jnp.concatenate([im, re], axis=1).astype(BF16))
    phases = jnp.concatenate(parts, axis=0)

    for h in range(2):
        row = iota((half, 4 * k_group), 0) + h * half
        source = (
            ((row // PIECE) % 2) * (2 * k_group) + ((row // (2 * PIECE)) % 2) * k_group + row // FOLD
        )
        chosen = jnp.where(iota((half, 4 * k_group), 1) == source, 1.0, 0.0).astype(BF16)
        ordered = mm(chosen, phases).astype(BF16)
        wide = mm(ordered, spread[...])
        same = iota((half, depth), 0) % PIECE == iota((half, depth), 1) % PIECE
        left4[pl.ds(h * half, half), :] = jnp.where(same, wide, 0.0).astype(BF16)

    for q in range(early, 2 * pieces):
        op_copy(q).start(priority=1)
    small[3].wait()
    pl.semaphore_wait(barrier, chips)

    def v_copy(s):
        to = peer(s)
        return pltpu.make_async_remote_copy(
            src_ref=vall.at[chip], dst_ref=vall.at[chip],
            send_sem=vs.at[to // 2], recv_sem=vr.at[chip],
            device_id={"row": to}, device_id_type=MESH,
        )

    for s in range(1, chips):
        v_copy(s).start()

    def v_wait(s):
        src = peer(s)
        pltpu.make_async_remote_copy(
            src_ref=vall.at[chip], dst_ref=vall.at[src // 2],
            send_sem=vs.at[src // 2], recv_sem=vr.at[src // 2],
            device_id={"row": src}, device_id_type=MESH,
        ).wait()

    def f_copy(t):
        return pltpu.make_async_remote_copy(
            src_ref=fsend.at[t], dst_ref=frecv.at[t], send_sem=fs.at[t], recv_sem=fr.at[t],
            device_id={"row": partner}, device_id_type=MESH,
        )

    def fourier(first, count):
        def body(i, carry):
            for u in range(UNROLL):
                for q in range(SPAN):
                    op_copy((first + i * UNROLL + u) * SPAN + q).wait()
            for u in range(UNROLL):
                t = first + i * UNROLL + u
                tiles = [
                    flat[pl.ds(pl.multiple_of((t * SPAN + q) * depth, depth), depth), :]
                    for q in range(SPAN)
                ]
                got = mm(left4[...], jnp.concatenate(tiles, axis=1))
                fown[t] = got[:half]
                fsend[t] = got[half:].astype(BF16)
            for u in range(UNROLL):
                f_copy(first + i * UNROLL + u).start()
            return carry

        lax.fori_loop(0, count // UNROLL, body, 0)

    def f_wait(op):
        def body(i, carry):
            f_copy(op * steps + i).wait()
            return carry

        lax.fori_loop(0, steps, body, 0)

    upper = iota((2 * PIECE, width), 0) < PIECE

    def left_turn(op, owner, kk):
        v_re, v_im = vall[owner, kk, 0], vall[owner, kk, 1]
        rows = pl.ds(pl.multiple_of((owner * per + kk) * FOLD, FOLD), FOLD)
        cells = [[[], []], [[], []]]
        for t in range(op * steps, (op + 1) * steps):
            total = fown[t, rows, :] + frecv[t, rows, :].astype(F32)
            for q in range(0, SPAN, 2):
                for part in range(2):
                    low = total[part * 8:part * 8 + 8, q * width:(q + 1) * width]
                    high = total[part * 8:part * 8 + 8, (q + 1) * width:(q + 2) * width]
                    cells[part][0].append(jnp.where(upper, low, pltpu.roll(high, PIECE, 0)))
                    cells[part][1].append(jnp.where(upper, pltpu.roll(low, PIECE, 0), high))
        high, low = split(
            jnp.concatenate(
                [
                    jnp.concatenate([jnp.concatenate(cells[part][c], axis=0) for c in range(2)], axis=1)
                    for part in range(2)
                ],
                axis=0,
            )
        )
        both = jnp.concatenate(
            [jnp.concatenate([v_re, v_im], axis=1), jnp.concatenate([-v_im, v_re], axis=1)], axis=0
        )
        return mm(jnp.concatenate([both, both], axis=1), jnp.concatenate([high, low], axis=0))

    def right_turn(g, owner, kk):
        v_re, v_im = vall[owner, kk, 0], vall[owner, kk, 1]
        g = g.astype(BF16)
        left = jnp.concatenate(
            [
                jnp.concatenate(
                    [g[p * bands:(p + 1) * bands, c * width:(c + 1) * width] for p in range(2)], axis=1
                )
                for c in range(2)
            ],
            axis=0,
        )
        right = jnp.concatenate(
            [jnp.concatenate([v_re, -v_im], axis=1), jnp.concatenate([v_im, v_re], axis=1)], axis=0
        )
        return mm(left, right, NT)

    def band_blocks(op, which):
        turned = [left_turn(op, owner, kk) for owner, kk in which]
        return [right_turn(g, owner, kk) for g, (owner, kk) in zip(turned, which)]

    def b_copy(op, kk, s):
        to = peer(s)
        return pltpu.make_async_remote_copy(
            src_ref=sbuf.at[op, kk, to // 2], dst_ref=rbuf.at[op, kk, chip],
            send_sem=bs.at[op, kk, to // 2], recv_sem=br.at[op, kk, chip],
            device_id={"row": to}, device_id_type=MESH,
        )

    def b_wait(op, kk, s):
        src = peer(s)
        pltpu.make_async_remote_copy(
            src_ref=sbuf.at[op, kk, src // 2], dst_ref=rbuf.at[op, kk, src // 2],
            send_sem=bs.at[op, kk, src // 2], recv_sem=br.at[op, kk, src // 2],
            device_id={"row": src}, device_id_type=MESH,
        ).wait()

    def bands_out(op, kk):
        owners = [peer(s) // 2 for s in range(1, chips)]
        for lot in range(0, chips - 1, LOT):
            some = owners[lot:lot + LOT]
            for to, b in zip(some, band_blocks(op, [(to, kk) for to in some])):
                sbuf[op, kk, to] = b.astype(BF16)
        for s in range(1, chips):
            b_copy(op, kk, s).start()

    def bands_own(op):
        for kk, b in enumerate(band_blocks(op, [(chip, kk) for kk in range(per)])):
            own[op, kk] = b

    fourier(0, steps)
    fourier(steps, steps // 2)
    for s in range(1, chips):
        v_wait(s)
    f_wait(0)
    bands_out(0, 0)
    fourier(steps + steps // 2, steps - steps // 2)
    for kk in range(1, per):
        bands_out(0, kk)
    bands_own(0)
    f_wait(1)
    for kk in range(per):
        bands_out(1, kk)
    bands_own(1)

    factor = 1.0 / math.sqrt(bands)

    def turn(m):
        return jnp.concatenate([-m[:, bands:], m[:, :bands]], axis=1)

    for kk in range(per):
        for op in range(2):
            for s in range(1, chips):
                b_wait(op, kk, s)
        sums = []
        for op in range(2):
            total = own[op, kk]
            for s in range(1, chips):
                total = total + rbuf[op, kk, peer(s) // 2].astype(F32)
            sums += [total[:bands], total[bands:]]
        ham, deriv, posit, last = sums
        i_deriv = turn(deriv)
        plus, minus = ham + i_deriv, ham - i_deriv
        lh, ll = split(jnp.concatenate([posit, minus], axis=1))
        rh, rl = split(jnp.concatenate([plus, turn(plus), posit, turn(posit)], axis=0))
        prod = mm(
            jnp.concatenate([lh, lh, ll], axis=1), jnp.concatenate([rh, rl, rh], axis=0)
        )
        res = last + factor * prod
        out_ref[kk, 0] = res[:, :bands]
        out_ref[kk, 1] = res[:, bands:]


def on_device(wannier_ops, r_coords, degeneracy, kpoints, bloch_vectors):
    n = lax.axis_size("row")
    chips = n // 2
    r_local, width = wannier_ops.shape[1], wannier_ops.shape[-1]
    per, _, bands, _ = bloch_vectors.shape
    r_pad = -(-r_local // 128) * 128
    pieces = width // PIECE
    steps = 2 * (pieces // SPAN)
    depth = 2 * PIECE * r_pad
    half = chips * per * FOLD
    ks = kpoints.shape[0]
    vmem = pl.BlockSpec(memory_space=pltpu.VMEM)
    far = pl.BlockSpec(memory_space=pl.ANY)
    dma = pltpu.SemaphoreType.DMA
    res = pl.pallas_call(
        functools.partial(kernel, n),
        out_shape=jax.ShapeDtypeStruct((per, 2, bands, bands), F32),
        in_specs=[far] * 5,
        out_specs=vmem,
        scratch_shapes=[
            pltpu.VMEM((2, pieces, r_pad, 2, PIECE, width), BF16),
            pltpu.VMEM((3, r_local), jnp.int32),
            pltpu.VMEM((1, r_local), jnp.int32),
            pltpu.VMEM((3, ks), jnp.int32),
            pltpu.VMEM((8, r_pad), F32),
            pltpu.VMEM((8, ks), F32),
            pltpu.VMEM((ks, r_pad), F32),
            pltpu.VMEM((n * per, r_pad), F32),
            pltpu.VMEM((2 * r_pad, depth), BF16),
            pltpu.VMEM((2 * half, depth), BF16),
            pltpu.VMEM((steps, half, SPAN * width), F32),
            pltpu.VMEM((steps, half, SPAN * width), BF16),
            pltpu.VMEM((steps, half, SPAN * width), BF16),
            pltpu.VMEM((chips, per, 2, bands, width), BF16),
            pltpu.VMEM((2, per, chips, 2 * bands, 2 * bands), BF16),
            pltpu.VMEM((2, per, chips, 2 * bands, 2 * bands), BF16),
            pltpu.VMEM((2, per, 2 * bands, 2 * bands), F32),
            dma((2 * pieces,)),
            dma((4,)),
            dma((steps,)),
            dma((steps,)),
            dma((chips,)),
            dma((chips,)),
            dma((2, per, chips)),
            dma((2, per, chips)),
        ],
        compiler_params=pltpu.CompilerParams(
            collective_id=0, has_side_effects=True, vmem_limit_bytes=62 * 1024 * 1024
        ),
    )(
        wannier_ops.reshape(2, r_local, 2, pieces, PIECE, width),
        r_coords.T, degeneracy.reshape(1, r_local), kpoints.T, bloch_vectors,
    )
    return res.reshape(per, 2, bands * bands)


def solution(mesh):
    in_specs = (
        P(None, "row", None, None, None),
        P("row", None),
        P("row"),
        P(),
        P(("op", "row"), None, None, None),
    )
    out_specs = P(("op", "row"), None, None)
    return jax.shard_map(
        on_device, mesh=mesh, in_specs=in_specs, out_specs=out_specs, check_vma=False
    )
```

```python
import functools
import math

import jax
import jax.numpy as jnp
from jax import lax
from jax.experimental import pallas as pl
from jax.experimental.pallas import tpu as pltpu
from jax.sharding import PartitionSpec as P

GRID = 16
RMAX = 8
TWO_PI = 6.283185307179586
PIECE = 4
SPAN = 4
UNROLL = 2
LOT = 3
EARLY = 24
FOLD = 4 * PIECE
MESH = pl.DeviceIdType.MESH
F32 = jnp.float32
BF16 = jnp.bfloat16
NT = (((1,), (1,)), ((), ()))
NN = (((1,), (0,)), ((), ()))
TN = (((0,), (0,)), ((), ()))


def mm(a, b, dims=NN):
    return lax.dot_general(a, b, dims, preferred_element_type=F32)


def split(x):
    high = x.astype(BF16)
    return high, (x - high.astype(F32)).astype(BF16)


def iota(shape, axis):
    return lax.broadcasted_iota(jnp.int32, shape, axis)


def kernel(
    n, ops_ref, rc_ref, deg_ref, kp_ref, v_ref, got_ref, own_ref,
    obuf, rci, degi, kpi, rcs, kps, inners, picked, spread, left4,
    fown, fsend, frecv, vall, sbuf, own,
    osem, isem, fs, fr, vs, vr, bs, br,
):
    me = lax.axis_index("row")
    group = lax.axis_index("op")
    core = lax.rem(me, 2)
    chip = me // 2
    partner = me + 1 - 2 * core
    chips = n // 2
    r_local, width = ops_ref.shape[1], ops_ref.shape[-1]
    r_pad = rcs.shape[1]
    pieces = width // PIECE
    steps = pieces // SPAN
    depth = 2 * PIECE * r_pad
    per, _, bands, _ = v_ref.shape
    slots = chips * per
    k_group = n * per
    half = slots * FOLD
    flat = obuf.reshape(2 * pieces * depth, width)

    tall = chips // 2
    offsets = [(a, b) for a in range(tall) for b in range(2) if a + b]
    offsets.sort(key=lambda step: -(min(step[0], 1) + step[1]))

    def shifted(d, sign):
        a, b = offsets[d]
        high = lax.rem(chip // 2 + sign * a + tall, tall)
        return 2 * high + lax.rem(lax.rem(chip, 2) + b, 2)

    def to_chip(d):
        return shifted(d, 1)

    def from_chip(d):
        return shifted(d, -1)

    def device(c):
        return {"row": 2 * c + core}

    others = range(len(offsets))

    barrier = pltpu.get_barrier_semaphore()
    pl.semaphore_signal(barrier, inc=1, device_id={"row": partner}, device_id_type=MESH)
    for d in others:
        pl.semaphore_signal(barrier, inc=1, device_id=device(to_chip(d)), device_id_type=MESH)

    small = [
        pltpu.make_async_copy(src, dst, isem.at[i])
        for i, (src, dst) in enumerate(
            ((kp_ref, kpi), (rc_ref, rci), (deg_ref, degi), (v_ref, vall.at[chip]))
        )
    ]
    for copy in small:
        copy.start()

    def op_copy(q):
        return pltpu.make_async_copy(
            ops_ref.at[q // pieces, :, :, q % pieces],
            obuf.at[q // pieces, q % pieces, pl.ds(0, r_local)],
            osem.at[q],
        )

    early = min(EARLY, 2 * pieces)
    for q in range(early):
        op_copy(q).start(priority=1)

    if r_pad > r_local:
        tail = 2 * PIECE * (r_pad - r_local)

        def clear(q, carry):
            flat[pl.ds(pl.multiple_of(q * depth, depth) + 2 * PIECE * r_local, tail), :] = jnp.zeros(
                (tail, width), BF16
            )
            return carry

        lax.fori_loop(0, 2 * pieces, clear, 0, unroll=4)

    for p in range(2):
        spread[pl.ds(p * r_pad, r_pad), :] = jnp.where(
            iota((r_pad, depth), 1) // PIECE == 2 * iota((r_pad, depth), 0) + p, 1.0, 0.0
        ).astype(BF16)
    rcs[...] = jnp.zeros_like(rcs)
    kps[...] = jnp.zeros_like(kps)

    for copy in small[:3]:
        copy.wait()
    rcs[pl.ds(0, 3), pl.ds(0, r_local)] = rci[...].astype(F32)
    kps[pl.ds(0, 3), :] = kpi[...].astype(F32)
    weights = jnp.concatenate(
        [1.0 / degi[...].astype(F32), jnp.zeros((1, r_pad - r_local), F32)], axis=1
    ) if r_pad > r_local else 1.0 / degi[...].astype(F32)
    inners[...] = mm(kps[...].astype(BF16), rcs[...].astype(BF16), TN)
    for h in range(2):
        for c in range(chips):
            owner = 2 * c + lax.rem(core + h, 2)
            picked[pl.ds((h * chips + c) * per, per), :] = inners[
                pl.ds(group * k_group + owner * per, per), :
            ]
    inner = picked[...]
    along_x = rcs[pl.ds(0, 1), :] / RMAX
    turns = inner - GRID * jnp.floor(inner / GRID)
    angles = turns * (TWO_PI / GRID)
    cosine = jnp.cos(angles) * weights
    sine = jnp.sin(angles) * weights
    parts = []
    for re, im in ((cosine, sine), (-along_x * sine, along_x * cosine)):
        parts.append(jnp.concatenate([re, -im], axis=1).astype(BF16))
        parts.append(jnp.concatenate([im, re], axis=1).astype(BF16))
    phases = jnp.concatenate(parts, axis=0)

    for h in range(2):
        row = iota((half, 4 * k_group), 0) + h * half
        source = (
            ((row // PIECE) % 2) * (2 * k_group) + ((row // (2 * PIECE)) % 2) * k_group + row // FOLD
        )
        chosen = jnp.where(iota((half, 4 * k_group), 1) == source, 1.0, 0.0).astype(BF16)
        ordered = mm(chosen, phases).astype(BF16)
        wide = mm(ordered, spread[...])
        same = iota((half, depth), 0) % PIECE == iota((half, depth), 1) % PIECE
        left4[pl.ds(h * half, half), :] = jnp.where(same, wide, 0.0).astype(BF16)

    for q in range(early, 2 * pieces):
        op_copy(q).start(priority=1)
    small[3].wait()
    pl.semaphore_wait(barrier, chips)

    def v_copy(d, landing):
        return pltpu.make_async_remote_copy(
            src_ref=vall.at[chip], dst_ref=vall.at[landing], send_sem=vs.at[d], recv_sem=vr.at[d],
            device_id=device(to_chip(d)), device_id_type=MESH,
        )

    for d in others:
        v_copy(d, chip).start()

    def f_copy(t):
        return pltpu.make_async_remote_copy(
            src_ref=fsend.at[t], dst_ref=frecv.at[t], send_sem=fs.at[t], recv_sem=fr.at[t],
            device_id={"row": partner}, device_id_type=MESH,
        )

    def fourier_lot(first, count, beside):
        for u in range(count * SPAN):
            op_copy(first * SPAN + u).wait()
        sums = []
        for u in range(count):
            tiles = [
                flat[pl.ds(pl.multiple_of(((first + u) * SPAN + q) * depth, depth), depth), :]
                for q in range(SPAN)
            ]
            sums.append(mm(left4[...], jnp.concatenate(tiles, axis=1)))
        turned = beside()
        for u, got in enumerate(sums):
            fown[first + u] = got[:half]
            fsend[first + u] = got[half:].astype(BF16)
        for u in range(count):
            f_copy(first + u).start()
        return turned

    def fourier(first, count):
        def body(i, carry):
            fourier_lot(first + i * UNROLL, UNROLL, lambda: None)
            return carry

        lax.fori_loop(0, count // UNROLL, body, 0)

    def f_wait(op):
        def body(i, carry):
            f_copy(op * steps + i).wait()
            return carry

        lax.fori_loop(0, steps, body, 0)

    upper = iota((2 * PIECE, width), 0) < PIECE

    def left_turn(op, owner, kk):
        v_re, v_im = vall[owner, kk, 0], vall[owner, kk, 1]
        rows = pl.ds(pl.multiple_of((owner * per + kk) * FOLD, FOLD), FOLD)
        cells = [[[], []], [[], []]]
        for t in range(op * steps, (op + 1) * steps):
            total = fown[t, rows, :] + frecv[t, rows, :].astype(F32)
            for q in range(0, SPAN, 2):
                for part in range(2):
                    low = total[part * 8:part * 8 + 8, q * width:(q + 1) * width]
                    high = total[part * 8:part * 8 + 8, (q + 1) * width:(q + 2) * width]
                    cells[part][0].append(jnp.where(upper, low, pltpu.roll(high, PIECE, 0)))
                    cells[part][1].append(jnp.where(upper, pltpu.roll(low, PIECE, 0), high))
        high, low = split(
            jnp.concatenate(
                [
                    jnp.concatenate([jnp.concatenate(cells[part][c], axis=0) for c in range(2)], axis=1)
                    for part in range(2)
                ],
                axis=0,
            )
        )
        both = jnp.concatenate(
            [jnp.concatenate([v_re, v_im], axis=1), jnp.concatenate([-v_im, v_re], axis=1)], axis=0
        )
        return mm(jnp.concatenate([both, both], axis=1), jnp.concatenate([high, low], axis=0))

    def right_turn(g, owner, kk):
        v_re, v_im = vall[owner, kk, 0], vall[owner, kk, 1]
        g = g.astype(BF16)
        left = jnp.concatenate(
            [
                jnp.concatenate(
                    [g[p * bands:(p + 1) * bands, c * width:(c + 1) * width] for p in range(2)], axis=1
                )
                for c in range(2)
            ],
            axis=0,
        )
        right = jnp.concatenate(
            [jnp.concatenate([v_re, -v_im], axis=1), jnp.concatenate([v_im, v_re], axis=1)], axis=0
        )
        return mm(left, right, NT)

    def band_blocks(op, which):
        turned = [left_turn(op, owner, kk) for owner, kk in which]
        return [right_turn(g, owner, kk) for g, (owner, kk) in zip(turned, which)]

    def b_copy(op, kk, d):
        return pltpu.make_async_remote_copy(
            src_ref=sbuf.at[op, kk, d], dst_ref=got_ref.at[op, kk, d],
            send_sem=bs.at[op, kk, d], recv_sem=br.at[op, kk, d],
            device_id=device(to_chip(d)), device_id_type=MESH,
        )

    def bands_out(op, kk, first, made=0):
        for d in others[:made]:
            b_copy(op, kk, d).start()
        lots = [] if made else [others[:first]]
        lots += [others[at:at + LOT] for at in range(first, len(others), LOT)]
        for lot in lots:
            for d, b in zip(lot, band_blocks(op, [(to_chip(d), kk) for d in lot])):
                sbuf[op, kk, d] = b.astype(BF16)
            for d in lot:
                b_copy(op, kk, d).start()

    def own_copy(op):
        return pltpu.make_async_copy(own.at[op], own_ref.at[op], isem.at[4 + op])

    def bands_own(op):
        for kk, b in enumerate(band_blocks(op, [(chip, kk) for kk in range(per)])):
            own[op, kk] = b
        own_copy(op).start()

    fourier(0, steps)
    fourier(steps, steps // 2)
    for d in others:
        v_copy(d, from_chip(d)).wait()
    f_wait(0)
    done = steps + steps // 2
    mates = [(to_chip(d), 0) for d in others[:LOT]]
    for d, b in enumerate(fourier_lot(done, UNROLL, lambda: band_blocks(0, mates))):
        sbuf[0, 0, d] = b.astype(BF16)
    bands_out(0, 0, LOT, LOT)
    fourier(done + UNROLL, 2 * steps - done - UNROLL)
    for kk in range(1, per):
        bands_out(0, kk, LOT)
    bands_own(0)
    f_wait(1)
    bands_out(1, 0, 1)
    for kk in range(1, per):
        bands_out(1, kk, LOT)
    bands_own(1)
    for kk in range(per):
        for op in range(2):
            for d in others:
                b_copy(op, kk, d).wait()
    for op in range(2):
        own_copy(op).wait()


def finish(got_ref, own_ref, out_ref, got, own, whole, flat, gsem, wsem, tsem):
    per, lanes = own.shape[1], own.shape[-1]
    bands = lanes // 2
    factor = 1.0 / math.sqrt(bands)

    def fetch(kk):
        return (
            pltpu.make_async_copy(got_ref.at[:, kk], got.at[:, kk], gsem.at[kk]),
            pltpu.make_async_copy(own_ref.at[:, kk], own.at[:, kk], wsem.at[kk]),
        )

    for kk in range(per):
        for copy in fetch(kk):
            copy.start()

    def turn(m):
        return jnp.concatenate([-m[:, bands:], m[:, :bands]], axis=1)

    for kk in range(per):
        for copy in fetch(kk):
            copy.wait()
    pairs = []
    for kk in range(per):
        sums = []
        for op in range(2):
            total = own[op, kk]
            for d in range(got.shape[2]):
                total = total + got[op, kk, d].astype(F32)
            sums += [total[:bands], total[bands:]]
        ham, deriv, posit, last = sums
        i_deriv = turn(deriv)
        plus, minus = ham + i_deriv, ham - i_deriv
        lh, ll = split(jnp.concatenate([posit, minus], axis=1))
        rh, rl = split(jnp.concatenate([plus, turn(plus), posit, turn(posit)], axis=0))
        prod = mm(
            jnp.concatenate([lh, lh, ll], axis=1), jnp.concatenate([rh, rl, rh], axis=0)
        )
        pairs.append((last, prod))
    for kk, (last, prod) in enumerate(pairs):
        whole[kk] = last + factor * prod
    for kk in range(per):
        even = whole[kk, pl.ds(0, bands // 2, stride=2), :]
        odd = whole[kk, pl.ds(1, bands // 2, stride=2), :]
        flat[kk, pl.ds(0, bands // 2, stride=2), :] = jnp.concatenate(
            [even[:, :bands], odd[:, :bands]], axis=1
        )
        flat[kk, pl.ds(1, bands // 2, stride=2), :] = jnp.concatenate(
            [even[:, bands:], odd[:, bands:]], axis=1
        )
    put = pltpu.make_async_copy(flat, out_ref, tsem)
    put.start()
    put.wait()


def on_device(wannier_ops, r_coords, degeneracy, kpoints, bloch_vectors):
    n = lax.axis_size("row")
    chips = n // 2
    r_local, width = wannier_ops.shape[1], wannier_ops.shape[-1]
    per, _, bands, _ = bloch_vectors.shape
    r_pad = -(-r_local // 128) * 128
    pieces = width // PIECE
    steps = 2 * (pieces // SPAN)
    depth = 2 * PIECE * r_pad
    half = chips * per * FOLD
    ks = kpoints.shape[0]
    far = pl.BlockSpec(memory_space=pl.ANY)
    dma = pltpu.SemaphoreType.DMA
    square = (2 * bands, 2 * bands)
    sums = pl.pallas_call(
        functools.partial(kernel, n),
        out_shape=(
            jax.ShapeDtypeStruct((2, per, chips - 1) + square, BF16),
            jax.ShapeDtypeStruct((2, per) + square, F32),
        ),
        in_specs=[far] * 5,
        out_specs=(far, far),
        scratch_shapes=[
            pltpu.VMEM((2, pieces, r_pad, 2, PIECE, width), BF16),
            pltpu.VMEM((3, r_local), jnp.int32),
            pltpu.VMEM((1, r_local), jnp.int32),
            pltpu.VMEM((3, ks), jnp.int32),
            pltpu.VMEM((8, r_pad), F32),
            pltpu.VMEM((8, ks), F32),
            pltpu.VMEM((ks, r_pad), F32),
            pltpu.VMEM((n * per, r_pad), F32),
            pltpu.VMEM((2 * r_pad, depth), BF16),
            pltpu.VMEM((2 * half, depth), BF16),
            pltpu.VMEM((steps, half, SPAN * width), F32),
            pltpu.VMEM((steps, half, SPAN * width), BF16),
            pltpu.VMEM((steps, half, SPAN * width), BF16),
            pltpu.VMEM((chips, per, 2, bands, width), BF16),
            pltpu.VMEM((2, per, chips - 1) + square, BF16),
            pltpu.VMEM((2, per) + square, F32),
            dma((2 * pieces,)),
            dma((6,)),
            dma((steps,)),
            dma((steps,)),
            dma((chips - 1,)),
            dma((chips - 1,)),
            dma((2, per, chips - 1)),
            dma((2, per, chips - 1)),
        ],
        compiler_params=pltpu.CompilerParams(
            collective_id=0, has_side_effects=True, vmem_limit_bytes=62 * 1024 * 1024
        ),
    )(
        wannier_ops.reshape(2, r_local, 2, pieces, PIECE, width),
        r_coords.T, degeneracy.reshape(1, r_local), kpoints.T, bloch_vectors,
    )
    res = pl.pallas_call(
        finish,
        out_shape=jax.ShapeDtypeStruct((per, bands, 2 * bands), F32),
        in_specs=[far] * 2,
        out_specs=far,
        scratch_shapes=[
            pltpu.VMEM((2, per, chips - 1) + square, BF16),
            pltpu.VMEM((2, per) + square, F32),
            pltpu.VMEM((per, bands, 2 * bands), F32),
            pltpu.VMEM((per, bands, 2 * bands), F32),
            dma((per,)),
            dma((per,)),
            dma,
        ],
        compiler_params=pltpu.CompilerParams(vmem_limit_bytes=62 * 1024 * 1024),
    )(*sums)
    res = res.reshape(per, bands * bands // width, 2, width).transpose(0, 2, 1, 3)
    return res.reshape(per, 2, bands * bands)


def solution(mesh):
    in_specs = (
        P(None, "row", None, None, None),
        P("row", None),
        P("row"),
        P(),
        P(("op", "row"), None, None, None),
    )
    out_specs = P(("op", "row"), None, None)
    return jax.shard_map(
        on_device, mesh=mesh, in_specs=in_specs, out_specs=out_specs, check_vma=False
    )
```

```python
import functools
import math

import jax
import jax.numpy as jnp
from jax import lax
from jax.experimental import pallas as pl
from jax.experimental.pallas import tpu as pltpu
from jax.sharding import PartitionSpec as P

GRID = 16
RMAX = 8
TWO_PI = 6.283185307179586
PIECE = 4
SPAN = 4
UNROLL = 2
LOT = 3
EARLY = 24
FOLD = 4 * PIECE
MESH = pl.DeviceIdType.MESH
F32 = jnp.float32
BF16 = jnp.bfloat16
NT = (((1,), (1,)), ((), ()))
NN = (((1,), (0,)), ((), ()))
TN = (((0,), (0,)), ((), ()))


def mm(a, b, dims=NN):
    return lax.dot_general(a, b, dims, preferred_element_type=F32)


def split(x):
    high = x.astype(BF16)
    return high, (x - high.astype(F32)).astype(BF16)


def iota(shape, axis):
    return lax.broadcasted_iota(jnp.int32, shape, axis)


def kernel(
    n, ops_ref, rc_ref, deg_ref, kp_ref, v_ref, got_ref, own_ref,
    obuf, rci, degi, kpi, rcs, kps, inners, picked, spread, left4,
    fown, fsend, frecv, vall, sbuf, own,
    osem, isem, fs, fr, vs, vr, bs, br,
):
    me = lax.axis_index("row")
    group = lax.axis_index("op")
    core = lax.rem(me, 2)
    chip = me // 2
    partner = me + 1 - 2 * core
    chips = n // 2
    r_local, width = ops_ref.shape[1], ops_ref.shape[-1]
    r_pad = rcs.shape[1]
    pieces = width // PIECE
    steps = pieces // SPAN
    depth = 2 * PIECE * r_pad
    per, _, bands, _ = v_ref.shape
    slots = chips * per
    k_group = n * per
    half = slots * FOLD
    flat = obuf.reshape(2 * pieces * depth, width)

    tall = chips // 2
    offsets = [(a, b) for a in range(tall) for b in range(2) if a + b]
    offsets.sort(key=lambda step: -(min(step[0], 1) + step[1]))

    def shifted(d, sign):
        a, b = offsets[d]
        high = lax.rem(chip // 2 + sign * a + tall, tall)
        return 2 * high + lax.rem(lax.rem(chip, 2) + b, 2)

    def to_chip(d):
        return shifted(d, 1)

    def from_chip(d):
        return shifted(d, -1)

    def device(c):
        return {"row": 2 * c + core}

    others = range(len(offsets))

    barrier = pltpu.get_barrier_semaphore()
    pl.semaphore_signal(barrier, inc=1, device_id={"row": partner}, device_id_type=MESH)
    for d in others:
        pl.semaphore_signal(barrier, inc=1, device_id=device(to_chip(d)), device_id_type=MESH)

    small = [
        pltpu.make_async_copy(src, dst, isem.at[i])
        for i, (src, dst) in enumerate(
            ((kp_ref, kpi), (rc_ref, rci), (deg_ref, degi), (v_ref, vall.at[chip]))
        )
    ]
    for copy in small:
        copy.start()

    def op_copy(q):
        return pltpu.make_async_copy(
            ops_ref.at[q // pieces, :, :, q % pieces],
            obuf.at[q // pieces, q % pieces, pl.ds(0, r_local)],
            osem.at[q],
        )

    early = min(EARLY, 2 * pieces)
    for q in range(early):
        op_copy(q).start(priority=1)

    if r_pad > r_local:
        tail = 2 * PIECE * (r_pad - r_local)

        def clear(q, carry):
            flat[pl.ds(pl.multiple_of(q * depth, depth) + 2 * PIECE * r_local, tail), :] = jnp.zeros(
                (tail, width), BF16
            )
            return carry

        lax.fori_loop(0, 2 * pieces, clear, 0, unroll=4)

    for p in range(2):
        spread[pl.ds(p * r_pad, r_pad), :] = jnp.where(
            iota((r_pad, depth), 1) // PIECE == 2 * iota((r_pad, depth), 0) + p, 1.0, 0.0
        ).astype(BF16)
    rcs[...] = jnp.zeros_like(rcs)
    kps[...] = jnp.zeros_like(kps)

    for copy in small[:3]:
        copy.wait()
    rcs[pl.ds(0, 3), pl.ds(0, r_local)] = rci[...].astype(F32)
    kps[pl.ds(0, 3), :] = kpi[...].astype(F32)
    weights = jnp.concatenate(
        [1.0 / degi[...].astype(F32), jnp.zeros((1, r_pad - r_local), F32)], axis=1
    ) if r_pad > r_local else 1.0 / degi[...].astype(F32)
    inners[...] = mm(kps[...].astype(BF16), rcs[...].astype(BF16), TN)
    for h in range(2):
        for c in range(chips):
            owner = 2 * c + lax.rem(core + h, 2)
            picked[pl.ds((h * chips + c) * per, per), :] = inners[
                pl.ds(group * k_group + owner * per, per), :
            ]
    inner = picked[...]
    along_x = rcs[pl.ds(0, 1), :] / RMAX
    turns = inner - GRID * jnp.floor(inner / GRID)
    angles = turns * (TWO_PI / GRID)
    cosine = jnp.cos(angles) * weights
    sine = jnp.sin(angles) * weights
    parts = []
    for re, im in ((cosine, sine), (-along_x * sine, along_x * cosine)):
        parts.append(jnp.concatenate([re, -im], axis=1).astype(BF16))
        parts.append(jnp.concatenate([im, re], axis=1).astype(BF16))
    phases = jnp.concatenate(parts, axis=0)

    for h in range(2):
        row = iota((half, 4 * k_group), 0) + h * half
        source = (
            ((row // PIECE) % 2) * (2 * k_group) + ((row // (2 * PIECE)) % 2) * k_group + row // FOLD
        )
        chosen = jnp.where(iota((half, 4 * k_group), 1) == source, 1.0, 0.0).astype(BF16)
        ordered = mm(chosen, phases).astype(BF16)
        wide = mm(ordered, spread[...])
        same = iota((half, depth), 0) % PIECE == iota((half, depth), 1) % PIECE
        left4[pl.ds(h * half, half), :] = jnp.where(same, wide, 0.0).astype(BF16)

    for q in range(early, 2 * pieces):
        op_copy(q).start(priority=1)
    small[3].wait()
    pl.semaphore_wait(barrier, chips)

    def v_copy(d, landing):
        return pltpu.make_async_remote_copy(
            src_ref=vall.at[chip], dst_ref=vall.at[landing], send_sem=vs.at[d], recv_sem=vr.at[d],
            device_id=device(to_chip(d)), device_id_type=MESH,
        )

    for d in others:
        v_copy(d, chip).start()

    def f_copy(t):
        return pltpu.make_async_remote_copy(
            src_ref=fsend.at[t], dst_ref=frecv.at[t], send_sem=fs.at[t], recv_sem=fr.at[t],
            device_id={"row": partner}, device_id_type=MESH,
        )

    def fourier_lot(first, count, beside):
        for u in range(count * SPAN):
            op_copy(first * SPAN + u).wait()
        sums = []
        for u in range(count):
            tiles = [
                flat[pl.ds(pl.multiple_of(((first + u) * SPAN + q) * depth, depth), depth), :]
                for q in range(SPAN)
            ]
            sums.append(mm(left4[...], jnp.concatenate(tiles, axis=1)))
        turned = beside()
        for u, got in enumerate(sums):
            fown[first + u] = got[:half]
            fsend[first + u] = got[half:].astype(BF16)
        for u in range(count):
            f_copy(first + u).start()
        return turned

    def fourier(first, count):
        def body(i, carry):
            fourier_lot(first + i * UNROLL, UNROLL, lambda: None)
            return carry

        lax.fori_loop(0, count // UNROLL, body, 0)

    def f_wait(op):
        def body(i, carry):
            f_copy(op * steps + i).wait()
            return carry

        lax.fori_loop(0, steps, body, 0)

    upper = iota((2 * PIECE, width), 0) < PIECE

    def left_turn(op, owner, kk):
        v_re, v_im = vall[owner, kk, 0], vall[owner, kk, 1]
        rows = pl.ds(pl.multiple_of((owner * per + kk) * FOLD, FOLD), FOLD)
        cells = [[[], []], [[], []]]
        for t in range(op * steps, (op + 1) * steps):
            total = fown[t, rows, :] + frecv[t, rows, :].astype(F32)
            for q in range(0, SPAN, 2):
                for part in range(2):
                    low = total[part * 8:part * 8 + 8, q * width:(q + 1) * width]
                    high = total[part * 8:part * 8 + 8, (q + 1) * width:(q + 2) * width]
                    cells[part][0].append(jnp.where(upper, low, pltpu.roll(high, PIECE, 0)))
                    cells[part][1].append(jnp.where(upper, pltpu.roll(low, PIECE, 0), high))
        high, low = split(
            jnp.concatenate(
                [
                    jnp.concatenate([jnp.concatenate(cells[part][c], axis=0) for c in range(2)], axis=1)
                    for part in range(2)
                ],
                axis=0,
            )
        )
        both = jnp.concatenate(
            [jnp.concatenate([v_re, v_im], axis=1), jnp.concatenate([-v_im, v_re], axis=1)], axis=0
        )
        return mm(jnp.concatenate([both, both], axis=1), jnp.concatenate([high, low], axis=0))

    def right_turn(g, owner, kk):
        v_re, v_im = vall[owner, kk, 0], vall[owner, kk, 1]
        g = g.astype(BF16)
        left = jnp.concatenate(
            [
                jnp.concatenate(
                    [g[p * bands:(p + 1) * bands, c * width:(c + 1) * width] for p in range(2)], axis=1
                )
                for c in range(2)
            ],
            axis=0,
        )
        right = jnp.concatenate(
            [jnp.concatenate([v_re, -v_im], axis=1), jnp.concatenate([v_im, v_re], axis=1)], axis=0
        )
        return mm(left, right, NT)

    def band_blocks(op, which):
        turned = [left_turn(op, owner, kk) for owner, kk in which]
        return [right_turn(g, owner, kk) for g, (owner, kk) in zip(turned, which)]

    def b_copy(op, kk, d):
        return pltpu.make_async_remote_copy(
            src_ref=sbuf.at[op, kk, d], dst_ref=got_ref.at[op, kk, d],
            send_sem=bs.at[op, kk, d], recv_sem=br.at[op, kk, d],
            device_id=device(to_chip(d)), device_id_type=MESH,
        )

    def bands_out(op, kk, first, made=0):
        for d in others[:made]:
            b_copy(op, kk, d).start()
        lots = [] if made else [others[:first]]
        lots += [others[at:at + LOT] for at in range(first, len(others), LOT)]
        for lot in lots:
            for d, b in zip(lot, band_blocks(op, [(to_chip(d), kk) for d in lot])):
                sbuf[op, kk, d] = b.astype(BF16)
            for d in lot:
                b_copy(op, kk, d).start()

    def own_copy(op):
        return pltpu.make_async_copy(own.at[op], own_ref.at[op], isem.at[4 + op])

    def bands_own(op):
        for kk, b in enumerate(band_blocks(op, [(chip, kk) for kk in range(per)])):
            own[op, kk] = b
        own_copy(op).start()

    fourier(0, steps)
    fourier(steps, steps // 2)
    for d in others:
        v_copy(d, from_chip(d)).wait()
    f_wait(0)
    done = steps + steps // 2
    mates = [(to_chip(d), 0) for d in others[:LOT]]
    for d, b in enumerate(fourier_lot(done, UNROLL, lambda: band_blocks(0, mates))):
        sbuf[0, 0, d] = b.astype(BF16)
    bands_out(0, 0, LOT, LOT)
    fourier(done + UNROLL, 2 * steps - done - UNROLL)
    for kk in range(1, per):
        bands_out(0, kk, LOT)
    bands_own(0)
    f_wait(1)
    bands_out(1, 0, 1)
    for kk in range(1, per):
        bands_out(1, kk, LOT)
    bands_own(1)
    for kk in range(per):
        for op in range(2):
            for d in others:
                b_copy(op, kk, d).wait()
    for op in range(2):
        own_copy(op).wait()


def finish(got_ref, own_ref, out_ref, got, own, whole, flat, gsem, wsem, tsem):
    per, lanes = own.shape[1], own.shape[-1]
    bands = lanes // 2
    factor = 1.0 / math.sqrt(bands)

    def fetch(kk):
        return (
            pltpu.make_async_copy(got_ref.at[:, kk], got.at[:, kk], gsem.at[kk]),
            pltpu.make_async_copy(own_ref.at[:, kk], own.at[:, kk], wsem.at[kk]),
        )

    for kk in range(per):
        for copy in fetch(kk):
            copy.start()

    def turn(m):
        return jnp.concatenate([-m[:, bands:], m[:, :bands]], axis=1)

    for kk in range(per):
        for copy in fetch(kk):
            copy.wait()
    pairs = []
    for kk in range(per):
        sums = []
        for op in range(2):
            total = own[op, kk]
            for d in range(got.shape[2]):
                total = total + got[op, kk, d].astype(F32)
            sums += [total[:bands], total[bands:]]
        ham, deriv, posit, last = sums
        i_ham, i_deriv = turn(ham), turn(deriv)
        plus, minus, i_plus = ham + i_deriv, ham - i_deriv, i_ham - deriv
        lh, ll = split(jnp.concatenate([posit, minus], axis=1))
        rh, rl = split(jnp.concatenate([plus, i_plus, posit, turn(posit)], axis=0))
        prod = mm(
            jnp.concatenate([lh, lh, ll], axis=1), jnp.concatenate([rh, rl, rh], axis=0)
        )
        pairs.append((last, prod))
    for kk, (last, prod) in enumerate(pairs):
        whole[kk] = last + factor * prod
    for kk in range(per):
        even = whole[kk, pl.ds(0, bands // 2, stride=2), :]
        odd = whole[kk, pl.ds(1, bands // 2, stride=2), :]
        flat[kk, pl.ds(0, bands // 2, stride=2), :] = jnp.concatenate(
            [even[:, :bands], odd[:, :bands]], axis=1
        )
        flat[kk, pl.ds(1, bands // 2, stride=2), :] = jnp.concatenate(
            [even[:, bands:], odd[:, bands:]], axis=1
        )
    put = pltpu.make_async_copy(flat, out_ref, tsem)
    put.start()
    put.wait()


def on_device(wannier_ops, r_coords, degeneracy, kpoints, bloch_vectors):
    n = lax.axis_size("row")
    chips = n // 2
    r_local, width = wannier_ops.shape[1], wannier_ops.shape[-1]
    per, _, bands, _ = bloch_vectors.shape
    r_pad = -(-r_local // 128) * 128
    pieces = width // PIECE
    steps = 2 * (pieces // SPAN)
    depth = 2 * PIECE * r_pad
    half = chips * per * FOLD
    ks = kpoints.shape[0]
    far = pl.BlockSpec(memory_space=pl.ANY)
    dma = pltpu.SemaphoreType.DMA
    square = (2 * bands, 2 * bands)
    sums = pl.pallas_call(
        functools.partial(kernel, n),
        out_shape=(
            jax.ShapeDtypeStruct((2, per, chips - 1) + square, BF16),
            jax.ShapeDtypeStruct((2, per) + square, F32),
        ),
        in_specs=[far] * 5,
        out_specs=(far, far),
        scratch_shapes=[
            pltpu.VMEM((2, pieces, r_pad, 2, PIECE, width), BF16),
            pltpu.VMEM((3, r_local), jnp.int32),
            pltpu.VMEM((1, r_local), jnp.int32),
            pltpu.VMEM((3, ks), jnp.int32),
            pltpu.VMEM((8, r_pad), F32),
            pltpu.VMEM((8, ks), F32),
            pltpu.VMEM((ks, r_pad), F32),
            pltpu.VMEM((n * per, r_pad), F32),
            pltpu.VMEM((2 * r_pad, depth), BF16),
            pltpu.VMEM((2 * half, depth), BF16),
            pltpu.VMEM((steps, half, SPAN * width), F32),
            pltpu.VMEM((steps, half, SPAN * width), BF16),
            pltpu.VMEM((steps, half, SPAN * width), BF16),
            pltpu.VMEM((chips, per, 2, bands, width), BF16),
            pltpu.VMEM((2, per, chips - 1) + square, BF16),
            pltpu.VMEM((2, per) + square, F32),
            dma((2 * pieces,)),
            dma((6,)),
            dma((steps,)),
            dma((steps,)),
            dma((chips - 1,)),
            dma((chips - 1,)),
            dma((2, per, chips - 1)),
            dma((2, per, chips - 1)),
        ],
        compiler_params=pltpu.CompilerParams(
            collective_id=0, has_side_effects=True, vmem_limit_bytes=62 * 1024 * 1024
        ),
    )(
        wannier_ops.reshape(2, r_local, 2, pieces, PIECE, width),
        r_coords.T, degeneracy.reshape(1, r_local), kpoints.T, bloch_vectors,
    )
    res = pl.pallas_call(
        finish,
        out_shape=jax.ShapeDtypeStruct((per, bands, 2 * bands), F32),
        in_specs=[far] * 2,
        out_specs=far,
        scratch_shapes=[
            pltpu.VMEM((2, per, chips - 1) + square, BF16),
            pltpu.VMEM((2, per) + square, F32),
            pltpu.VMEM((per, bands, 2 * bands), F32),
            pltpu.VMEM((per, bands, 2 * bands), F32),
            dma((per,)),
            dma((per,)),
            dma,
        ],
        compiler_params=pltpu.CompilerParams(vmem_limit_bytes=62 * 1024 * 1024),
    )(*sums)
    res = res.reshape(per, bands * bands // width, 2, width).transpose(0, 2, 1, 3)
    return res.reshape(per, 2, bands * bands)


def solution(mesh):
    in_specs = (
        P(None, "row", None, None, None),
        P("row", None),
        P("row"),
        P(),
        P(("op", "row"), None, None, None),
    )
    out_specs = P(("op", "row"), None, None)
    return jax.shard_map(
        on_device, mesh=mesh, in_specs=in_specs, out_specs=out_specs, check_vma=False
    )
```
